256 devices in a mesh: zero: 16 (over y, x), width: 16 (over z, core).
Axes of the slice: x: 4, y: 4, z: 8, core: 2. Of those that a mesh axis runs over, the one named last changes fastest.
Arguments:
- train_gate: float32 [5120, 13824], P('zero', 'width'), may hold values from -0.125 to 0.125
- drift_gate: float32 [5120, 13824], P('zero', 'width'), may hold values from -0.078125 to 0.078125
- spread_gate: float32 [5120, 13824], P('zero', 'width'), may hold values from -0.078125 to 0.078125
- train_up: float32 [5120, 13824], P('zero', 'width'), may hold values from -0.125 to 0.125
- drift_up: float32 [5120, 13824], P('zero', 'width'), may hold values from -0.078125 to 0.078125
- spread_up: float32 [5120, 13824], P('zero', 'width'), may hold values from -0.078125 to 0.078125
- norm_gain: float32 [5120], P('zero'), may hold values from 0.25 to 1.75
Outputs:
- serving_gate: bfloat16 [5120, 13824], P(None, 'width')
- serving_up: bfloat16 [5120, 13824], P(None, 'width')
- factor_gate: float32 [13824], P('width')
- factor_up: float32 [13824], P('width')
The draws below stay inside these ranges and needn't reach their ends.
All inputs are finite; a program needn't handle non-finite values. Where the reference program divides by a largest or mean magnitude, that divisor is 1e-20 or more.
Results may differ from the reference program's by a relative error of at most 0.001.
Values may be sent and summed in bfloat16 or wider, within the bound.
No kernel may reach another device: no remote copies, remote signals or barrier semaphores. Data moves between devices by JAX's collectives and lax.ppermute only.
A program may use at most 192 MiB of HBM per device.

```python
import jax
import jax.numpy as jnp

D_MODEL = 5120
D_INNER = 13824


def spiked(values, key, source, target, blocks, factor):
    def block_of(axis_at):
        return (jnp.arange(values.shape[axis_at]) // (values.shape[axis_at] // blocks)).reshape((-1,) + (1,) * (values.ndim - 1 - axis_at))

    one_side = jax.random.permutation(key, blocks)[block_of(target)]
    second = (block_of(target) + blocks // 2) % blocks
    return jnp.where((block_of(source) == one_side) | (block_of(source) == second), factor * values, values)


def block_scale(key, dims, cuts, least, high):
    gain, own = 1.0, jax.random.fold_in(key, 6)
    for axis_at, blocks in cuts:
        steps = jnp.exp(jax.random.uniform(jax.random.fold_in(own, axis_at), (blocks,), jnp.float32, least / len(cuts), high / len(cuts)))
        gain = gain * jnp.repeat(steps, dims[axis_at] // blocks).reshape([-1 if axis == axis_at else 1 for axis in range(len(dims))])
    return gain


def normal_values(rng, extent, width, bound, cuts=(), kind=jnp.bfloat16):
    result = jax.random.normal(rng, extent, jnp.float32) * width
    if len(cuts) > 0:
        result = block_scale(rng, extent, cuts, -0.22, 0.18) * result
    return jnp.clip(result, min=-bound, max=bound).astype(kind)


def heavy_noise(own_key, dims, deviation, bound, cuts, heavy, held_as=jnp.bfloat16):
    array = deviation * jax.random.normal(own_key, dims, jnp.float32)
    if cuts:
        array = array * block_scale(own_key, dims, cuts, -0.22, 0.18)
    return jnp.clip(spiked(array, jax.random.fold_in(own_key, 3), *heavy), -bound, bound).astype(held_as)


def setup_inputs(seed: int = 0) -> dict:
    arg_keys = jax.random.split(jax.random.key(seed), 8)
    return {
        "train_gate": heavy_noise(arg_keys[0], (D_MODEL, D_INNER), D_MODEL ** -0.5, 0.125, ((0, 16), (1, 16)), (0, 1, 16, 2.0), jnp.float32),
        "drift_gate": normal_values(arg_keys[1], (D_MODEL, D_INNER), D_MODEL ** -0.5, 0.078125, ((0, 16), (1, 16)), jnp.float32),
        "spread_gate": normal_values(arg_keys[2], (D_MODEL, D_INNER), D_MODEL ** -0.5, 0.078125, ((0, 16), (1, 16)), jnp.float32),
        "train_up": heavy_noise(arg_keys[3], (D_MODEL, D_INNER), D_MODEL ** -0.5, 0.125, ((0, 16), (1, 16)), (0, 1, 16, 2.0), jnp.float32),
        "drift_up": normal_values(arg_keys[4], (D_MODEL, D_INNER), D_MODEL ** -0.5, 0.078125, ((0, 16), (1, 16)), jnp.float32),
        "spread_up": normal_values(arg_keys[5], (D_MODEL, D_INNER), D_MODEL ** -0.5, 0.078125, ((0, 16), (1, 16)), jnp.float32),
        "norm_gain": jnp.clip(1.0 + 0.15 * jax.random.normal(arg_keys[6], (D_MODEL,), jnp.float32), 0.25, 1.75),
    }


learn_rate = 0.3
hold_rate = 0.9


def reference(train_gate, drift_gate, spread_gate, train_up, drift_up, spread_up, norm_gain):
    hold_gate = hold_rate * drift_gate + spread_gate
    whole_gate = train_gate - learn_rate * hold_gate
    hold_up = hold_rate * drift_up + spread_up
    whole_up = train_up - learn_rate * hold_up
    whole_gained_gate = whole_gate * norm_gain[:, None]
    whole_gained_up = whole_up * norm_gain[:, None]
    factor_gate = jnp.max(jnp.abs(whole_gained_gate), axis=0)
    serving_gate = (whole_gained_gate / factor_gate).astype(jnp.bfloat16)
    factor_up = jnp.max(jnp.abs(whole_gained_up), axis=0)
    serving_up = (whole_gained_up / factor_up).astype(jnp.bfloat16)
    return serving_gate, serving_up, factor_gate, factor_up
```

```python
import functools

import jax
import jax.numpy as jnp
from jax import lax
from jax.experimental import pallas as pl
from jax.experimental.pallas import tpu as pltpu
from jax.sharding import PartitionSpec as P


learn_rate = 0.3
hold_rate = 0.9


ROWS = 320
COLS = 864
FULL = 256
HALF = 64
QUART = COLS // 4
PIECE = COLS + QUART
CUT = 544
SIDE = 4


def pack_kernel(w_ref, f_ref, o_ref):
    odd = lax.axis_index("zero") % 2
    full_at = pl.multiple_of(odd * HALF, 8)
    half_at = pl.multiple_of((1 - odd) * FULL, 8)
    for at in range(0, COLS, 128):
        n = min(128, COLS - at)
        f = f_ref[:, at : at + n]
        w = w_ref[pl.ds(full_at, FULL), at : at + n] / f
        o_ref[at : at + n, :] = w.T.astype(jnp.bfloat16)
    h = w_ref[pl.ds(half_at, HALF), :] / f_ref[...]
    t = jnp.concatenate([h, h], axis=0).T
    low = lax.broadcasted_iota(jnp.int32, (2 * QUART, 128), 1) < HALF
    keep = jnp.logical_xor(low, odd == 1)
    p = jnp.where(keep, t[: 2 * QUART], t[2 * QUART :]).astype(jnp.bfloat16)
    o_ref[COLS:, :128] = p[:QUART]
    o_ref[COLS:, 128:] = p[QUART:]


def packed(w, f):
    return pl.pallas_call(
        pack_kernel,
        out_shape=jax.ShapeDtypeStruct((PIECE, 256), jnp.bfloat16),
        in_specs=[pl.BlockSpec(memory_space=pltpu.VMEM)] * 2,
        out_specs=pl.BlockSpec(memory_space=pltpu.VMEM),
        compiler_params=pltpu.CompilerParams(vmem_limit_bytes=8 << 20),
        cost_estimate=pl.CostEstimate(flops=4_000_000, bytes_accessed=1_600_000, transcendentals=0),
    )(w, f.reshape(1, COLS))


def tile_of(kx, ky):
    i = lax.axis_index("zero")
    x, y = i % SIDE, i // SIDE
    j = ((y + SIDE - ky) % SIDE) * SIDE + (x + SIDE - kx) % SIDE
    return pl.multiple_of((5 * j + j % 2) // 2 * 128, 128)


def pair_tile(kx, ky):
    i = lax.axis_index("zero")
    x, y = i % SIDE, i // SIDE
    j = ((y + SIDE - ky) % SIDE) * SIDE + (x + SIDE - kx) % SIDE
    return pl.multiple_of((5 * (j // 2) + 2) * 128, 128)


def place_kernel(plan, n_in, first, *refs):
    ins, outs = refs[:n_in], refs[n_in + len(plan) * (not first) :][: len(plan)]
    tiles, sem_full, sem_tile = refs[-3:]
    odd = lax.axis_index("zero") % 2
    done = []
    for (layout, fulls, _), out in zip(plan, outs):
        for key in fulls:
            at = tile_of(*key)
            for r, a, b in layout[key]:
                hi = min(b, COLS)
                if hi > a:
                    c = pltpu.make_async_copy(
                        ins[r].at[pl.ds(0, hi - a), :], out.at[pl.ds(a, hi - a), pl.ds(at, FULL)], sem_full.at[len(done)]
                    )
                    c.start()
                    done.append(c)

    keep = jnp.logical_xor(lax.broadcasted_iota(jnp.int32, (QUART, 128), 1) < HALF, odd == 1)
    n_tiles = 0
    for (layout, _, pairs), out in zip(plan, outs):

        def half(key, lanes):
            r, a, _ = layout[key][-1]
            return ins[r][COLS - a : PIECE - a, lanes].astype(jnp.float32)

        for p, ky in pairs:
            tile = tiles.at[n_tiles]

            def join(kx):
                for b in range(2):
                    lanes = slice(128 * b, 128 * b + 128)
                    one, two = half((2 * p, ky), lanes), half((kx, ky), lanes)
                    top = jnp.where(keep, one, two)
                    low = pltpu.roll(jnp.where(keep, two, one), HALF, 1)
                    tile[QUART * b : QUART * b + QUART, :] = top.astype(jnp.bfloat16)
                    tile[QUART * b + 2 * QUART : QUART * b + 3 * QUART, :] = low.astype(jnp.bfloat16)

            pl.when(odd == 0)(lambda: join(3 - 2 * p))
            pl.when(odd == 1)(lambda: join(1 + 2 * p))
            c = pltpu.make_async_copy(tile, out.at[:, pl.ds(pair_tile(2 * p, ky), 128)], sem_tile.at[n_tiles])
            c.start()
            done.append(c)
            n_tiles += 1
    for c in done:
        c.wait()


def place(jobs):
    refs, plan = [], []
    for _, got, fulls, pairs in jobs:
        layout = {}
        for key in list(fulls) + [(k, ky) for p, ky in pairs for k in (2 * p, 1, 3)]:
            if key not in layout:
                layout[key], at = [], 0
                for part in got[key]:
                    layout[key].append((len(refs), at, at + part.shape[0]))
                    refs.append(part)
                    at += part.shape[0]
        plan.append((layout, tuple(fulls), tuple(pairs)))
    first = jobs[0][0] is None
    olds = [] if first else [j[0] for j in jobs]
    n_tiles = max(1, sum(len(j[3]) for j in jobs))
    n_full = max(1, sum(len(layout[k]) for layout, fulls, _ in plan for k in fulls))
    shape = jax.ShapeDtypeStruct((COLS, ROWS * SIDE * SIDE), jnp.bfloat16)
    return pl.pallas_call(
        functools.partial(place_kernel, plan, len(refs), first),
        out_shape=[shape] * len(jobs),
        in_specs=[pl.BlockSpec(memory_space=pltpu.VMEM)] * len(refs) + [pl.BlockSpec(memory_space=pl.ANY)] * len(olds),
        out_specs=[pl.BlockSpec(memory_space=pl.ANY)] * len(jobs),
        scratch_shapes=[
            pltpu.VMEM((n_tiles, COLS, 128), jnp.bfloat16),
            pltpu.SemaphoreType.DMA((n_full,)),
            pltpu.SemaphoreType.DMA((n_tiles,)),
        ],
        input_output_aliases={len(refs) + i: i for i in range(len(olds))},
        compiler_params=pltpu.CompilerParams(vmem_limit_bytes=16 << 20),
        cost_estimate=pl.CostEstimate(flops=1_000_000, bytes_accessed=4_000_000, transcendentals=0),
    )(*refs, *olds)


def shift(a, dx, dy):
    pairs = [
        (SIDE * y + x, SIDE * ((y + dy) % SIDE) + (x + dx) % SIDE) for y in range(SIDE) for x in range(SIDE)
    ]
    return lax.ppermute(a, "zero", pairs)


ORDER = [
    *"gs+0 gs-0 us+0 us-0".split(),
    *"ub+0 gb+0 ub-0 gb-0".split(),
    *"gt+1 gt-3 ut+1 ut-3".split(),
    *"ub+1 ub-3 gb+1 gb-3".split(),
    *"ub+3 gb+3".split(),
    *"ub-2a gb-2a ub-2b gb-2b".split(),
    *"ub+2a gb+2a ub+2b gb+2b".split(),
    *"ub-1 gb-1".split(),
    *"Pg0 Pu0".split(),
    *"uf+0 gf+0 uf-3 gf-3".split(),
    *"uf+1 gf+1 uf-2a gf-2a".split(),
    *"uf-2b gf-2b".split(),
    *"Pg1 Pu1 Pg3 Pu3".split(),
    *"Pg2 Pu2".split(),
    *"Pend".split(),
]


def spread(gate, up):
    small = {"g": {"0": gate}, "u": {"0": up}}
    large = {"g": {}, "u": {}}
    out = {"g": None, "u": None}

    def move(a, on_x, sign):
        d = 1 if sign == "+" else -1
        return shift(a, d, 0) if on_x else shift(a, 0, d)

    def pieces(m):
        parts = lambda get: {k: [get(q) for q in ("2a", "2b")] if k == 2 else [get(str(k))] for k in range(SIDE)}
        got = {}
        for step in range(SIDE):
            from_step = (lambda q: small[m][q]) if step == 0 else (lambda q: large[m].get((step, q)))
            for k, v in parts(from_step).items():
                got[(k, step) if m == "g" else (step, k)] = v
        return got

    def put(*jobs):
        res = place([(out[m], pieces(m), fulls, pairs) for m, fulls, pairs in jobs])
        for (m, _, _), r in zip(jobs, res):
            out[m] = r

    every = range(SIDE)
    kernels = {
        "Pg0": [("g", [(k, 0) for k in every], [(0, 0), (1, 0)])],
        "Pg1": [("g", [(k, 1) for k in every], [(0, 1), (1, 1)])],
        "Pg3": [("g", [(k, 3) for k in every], [(0, 3), (1, 3)])],
        "Pg2": [("g", [(0, 2), (3, 2)], [])],
        "Pu0": [("u", [(0, k) for k in every], [])],
        "Pu1": [("u", [(1, k) for k in every], [])],
        "Pu3": [("u", [(3, k) for k in every], [(0, k) for k in every])],
        "Pu2": [("u", [(2, 0), (2, 3)], [(1, 0), (1, 3)])],
        "Pend": [
            ("g", [(1, 2), (2, 2)], [(0, 2), (1, 2)]),
            ("u", [(2, 1), (2, 2)], [(1, 1), (1, 2)]),
        ],
    }
    for name in ORDER:
        if name[0] == "P":
            put(*kernels[name])
            continue
        m, kind, sign, q = name[0], name[1], name[2], name[3:]
        on_x = (m == "g") == (kind in "st")
        step = 1 if sign == "+" else 3
        if kind == "s":
            small[m][str(step)] = move(small[m]["0"], on_x, sign)
        elif kind == "t":
            part = small[m][q][:CUT] if sign == "+" else small[m][q][CUT:]
            small[m]["2a" if sign == "+" else "2b"] = move(part, on_x, sign)
        elif kind == "b":
            large[m][(step, q)] = move(small[m][q], on_x, sign)
        else:
            large[m][(2, q)] = move(large[m][(step, q)], on_x, sign)
    return out["g"], out["u"]


def sent_to_all(array, axis):
    count = lax.axis_size(axis)
    return lax.all_to_all(jnp.broadcast_to(array[None], (count, *array.shape)), axis, 0, 0, tiled=True)


def body(train_gate, drift_gate, spread_gate, train_up, drift_up, spread_up, norm_gain):
    hold_gate = hold_rate * drift_gate + spread_gate
    whole_gate = train_gate - learn_rate * hold_gate
    hold_up = hold_rate * drift_up + spread_up
    whole_up = train_up - learn_rate * hold_up
    gained_gate = whole_gate * norm_gain[:, None]
    gained_up = whole_up * norm_gain[:, None]
    tops = jnp.concatenate([jnp.max(jnp.abs(gained_gate), axis=0), jnp.max(jnp.abs(gained_up), axis=0)])
    tops = sent_to_all(tops, "zero").max(axis=0)
    factor_gate, factor_up = tops[:COLS], tops[COLS:]

    gate = packed(gained_gate, factor_gate)
    up = packed(gained_up, factor_up)
    serving_gate, serving_up = spread(gate, up)
    return serving_gate.T, serving_up.T, factor_gate, factor_up


def solution(mesh):
    return jax.shard_map(
        body,
        mesh=mesh,
        in_specs=(P("zero", "width"),) * 6 + (P("zero"),),
        out_specs=(P(None, "width"), P(None, "width"), P("width"), P("width")),
        check_vma=False,
    )
```

```python
import functools

import jax
import jax.numpy as jnp
from jax import lax
from jax.experimental import pallas as pl
from jax.experimental.pallas import tpu as pltpu
from jax.sharding import PartitionSpec as P


learn_rate = 0.3
hold_rate = 0.9


ROWS = 320
COLS = 864
FULL = 256
HALF = 64
QUART = COLS // 4
PIECE = COLS + QUART
CUT = 624
SIDE = 4


def pack_kernel(m, w_ref, tops_ref, o_ref):
    odd = lax.axis_index("zero") % 2
    full_at = pl.multiple_of(odd * HALF, 8)
    half_at = pl.multiple_of((1 - odd) * FULL, 8)
    factor = jnp.max(tops_ref[:, m, :], axis=0, keepdims=True)
    for at in range(0, COLS, 128):
        n = min(128, COLS - at)
        w = w_ref[pl.ds(full_at, FULL), at : at + n] / factor[:, at : at + n]
        o_ref[at : at + n, :] = w.T.astype(jnp.bfloat16)
    h = w_ref[pl.ds(half_at, HALF), :] / factor
    t = jnp.concatenate([h, h], axis=0).T
    low = lax.broadcasted_iota(jnp.int32, (2 * QUART, 128), 1) < HALF
    keep = jnp.logical_xor(low, odd == 1)
    p = jnp.where(keep, t[: 2 * QUART], t[2 * QUART :]).astype(jnp.bfloat16)
    o_ref[COLS:, :128] = p[:QUART]
    o_ref[COLS:, 128:] = p[QUART:]


def packed(w, tops, m):
    return pl.pallas_call(
        functools.partial(pack_kernel, m),
        out_shape=jax.ShapeDtypeStruct((PIECE, 256), jnp.bfloat16),
        in_specs=[pl.BlockSpec(memory_space=pltpu.VMEM)] * 2,
        out_specs=pl.BlockSpec(memory_space=pltpu.VMEM),
        compiler_params=pltpu.CompilerParams(vmem_limit_bytes=8 << 20),
        cost_estimate=pl.CostEstimate(flops=4_000_000, bytes_accessed=1_600_000, transcendentals=0),
    )(w, tops)


def tile_of(kx, ky):
    i = lax.axis_index("zero")
    x, y = i % SIDE, i // SIDE
    j = ((y + SIDE - ky) % SIDE) * SIDE + (x + SIDE - kx) % SIDE
    return pl.multiple_of((5 * j + j % 2) // 2 * 128, 128)


def pair_tile(kx, ky):
    i = lax.axis_index("zero")
    x, y = i % SIDE, i // SIDE
    j = ((y + SIDE - ky) % SIDE) * SIDE + (x + SIDE - kx) % SIDE
    return pl.multiple_of((5 * (j // 2) + 2) * 128, 128)


def place_kernel(plan, n_in, first, *refs):
    ins, outs = refs[:n_in], refs[n_in + len(plan) * (not first) :][: len(plan)]
    tiles, sem_full, sem_tile = refs[-3:]
    odd = lax.axis_index("zero") % 2
    done = []
    for (layout, fulls, _), out in zip(plan, outs):
        for key, part in fulls:
            at = tile_of(*key)
            for r, a, b in [layout[key, q] for q in part]:
                hi = min(b, COLS)
                if hi > a:
                    c = pltpu.make_async_copy(
                        ins[r].at[pl.ds(0, hi - a), :], out.at[pl.ds(a, hi - a), pl.ds(at, FULL)], sem_full.at[len(done)]
                    )
                    c.start()
                    done.append(c)

    keep = jnp.logical_xor(lax.broadcasted_iota(jnp.int32, (QUART, 128), 1) < HALF, odd == 1)
    n_tiles = 0
    for (layout, _, pairs), out in zip(plan, outs):

        def half(key, lanes):
            r, a, _ = layout[key, -1]
            return ins[r][COLS - a : PIECE - a, lanes].astype(jnp.float32)

        for p, ky in pairs:
            tile = tiles.at[n_tiles]

            def join(kx):
                for b in range(2):
                    lanes = slice(128 * b, 128 * b + 128)
                    one, two = half((2 * p, ky), lanes), half((kx, ky), lanes)
                    top = jnp.where(keep, one, two)
                    low = pltpu.roll(jnp.where(keep, two, one), HALF, 1)
                    tile[QUART * b : QUART * b + QUART, :] = top.astype(jnp.bfloat16)
                    tile[QUART * b + 2 * QUART : QUART * b + 3 * QUART, :] = low.astype(jnp.bfloat16)

            pl.when(odd == 0)(lambda: join(3 - 2 * p))
            pl.when(odd == 1)(lambda: join(1 + 2 * p))
            c = pltpu.make_async_copy(tile, out.at[:, pl.ds(pair_tile(2 * p, ky), 128)], sem_tile.at[n_tiles])
            c.start()
            done.append(c)
            n_tiles += 1
    for c in done:
        c.wait()


def place(jobs):
    refs, plan = [], []
    for _, got, fulls, pairs in jobs:
        layout = {}
        need = [(key, q) for key, part in fulls for q in part]
        need += [((k, ky), -1) for p, ky in pairs for k in (2 * p, 1, 3)]
        for key, q in need:
            parts = got[key]
            one = parts[q]
            if not any(one is r for r in refs):
                refs.append(one)
            r = [one is x for x in refs].index(True)
            at = sum(x.shape[0] for x in parts[: q % len(parts)])
            layout[key, q] = (r, at, at + one.shape[0])
        plan.append((layout, tuple(fulls), tuple(pairs)))
    first = jobs[0][0] is None
    olds = [] if first else [j[0] for j in jobs]
    n_tiles = max(1, sum(len(j[3]) for j in jobs))
    n_full = max(1, sum(len(part) for _, fulls, _ in plan for _, part in fulls))
    shape = jax.ShapeDtypeStruct((COLS, ROWS * SIDE * SIDE), jnp.bfloat16)
    return pl.pallas_call(
        functools.partial(place_kernel, plan, len(refs), first),
        out_shape=[shape] * len(jobs),
        in_specs=[pl.BlockSpec(memory_space=pltpu.VMEM)] * len(refs) + [pl.BlockSpec(memory_space=pl.ANY)] * len(olds),
        out_specs=[pl.BlockSpec(memory_space=pl.ANY)] * len(jobs),
        scratch_shapes=[
            pltpu.VMEM((n_tiles, COLS, 128), jnp.bfloat16),
            pltpu.SemaphoreType.DMA((n_full,)),
            pltpu.SemaphoreType.DMA((n_tiles,)),
        ],
        input_output_aliases={len(refs) + i: i for i in range(len(olds))},
        compiler_params=pltpu.CompilerParams(vmem_limit_bytes=6 << 20),
        cost_estimate=pl.CostEstimate(flops=1_000_000, bytes_accessed=4_000_000, transcendentals=0),
    )(*refs, *olds)


def shift(a, dx, dy):
    pairs = [
        (SIDE * y + x, SIDE * ((y + dy) % SIDE) + (x + dx) % SIDE) for y in range(SIDE) for x in range(SIDE)
    ]
    return lax.ppermute(a, "zero", pairs)


ORDER = [
    *"gs+0 us+0 gs-0 us-0".split(),
    *"ub+0 gb+0 ub-0 gb-0".split(),
    *"gt+1 ut+1 gt-3 ut-3".split(),
    *"ub+1 gb+1 ub-3 gb-3".split(),
    *"ub+3 gb+3".split(),
    *"ub-2a gb-2a ub-2b gb-2b".split(),
    *"ub+2a gb+2a ub+2b gb+2b".split(),
    *"ub-1 gb-1".split(),
    *"Pg0 Pu0".split(),
    *"uf+0 gf+0 uf-3 gf-3".split(),
    *"uf+1a gf+1a uf-2a gf-2a".split(),
    *"uf+1b gf+1b uf-2b gf-2b".split(),
    *"Pg1 Pu1 Pg3 Pu3".split(),
    *"Pg2 Pu2".split(),
    *"Pmid Pend".split(),
]


def spread(gate, up):
    small = {"g": {"0": gate}, "u": {"0": up}}
    large = {"g": {}, "u": {}}
    out = {"g": None, "u": None}

    def move(a, on_x, sign):
        d = 1 if sign == "+" else -1
        return shift(a, d, 0) if on_x else shift(a, 0, d)

    def pieces(m):
        got = {}
        for step in range(SIDE):
            have = small[m] if step == 0 else {q: v for (s, q), v in large[m].items() if s == step}
            for k in range(SIDE):
                names = [str(k)] if str(k) in have else [f"{k}a", f"{k}b"]
                got[(k, step) if m == "g" else (step, k)] = [have.get(q) for q in names]
        return got

    def whole(m, keys):
        return [(key, tuple(range(len(pieces(m)[key])) if (pieces(m)[key][0] is not None) else ())) for key in keys]

    def put(name, *jobs):
        split = {"Pmid": (0,), "Pend": (1,)}
        res = place(
            [
                (out[m], pieces(m), [(k, split[name]) if name in split else w for k, w in zip(keys, whole(m, keys))], pairs)
                for m, keys, pairs in jobs
            ],
        )
        for (m, _, _), r in zip(jobs, res):
            out[m] = r

    every = range(SIDE)
    kernels = {
        "Pg0": [("g", [(k, 0) for k in every], [(0, 0), (1, 0)])],
        "Pg1": [("g", [(k, 1) for k in every], [(0, 1), (1, 1)])],
        "Pg3": [("g", [(k, 3) for k in every], [(0, 3), (1, 3)])],
        "Pg2": [("g", [(0, 2), (3, 2)], [])],
        "Pu0": [("u", [(0, k) for k in every], [])],
        "Pu1": [("u", [(1, k) for k in every], [])],
        "Pu3": [("u", [(3, k) for k in every], [(0, k) for k in every])],
        "Pu2": [("u", [(2, 0), (2, 3)], [(1, 0), (1, 3)])],
        "Pmid": [("g", [(1, 2), (2, 2)], []), ("u", [(2, 1), (2, 2)], [])],
        "Pend": [
            ("g", [(1, 2), (2, 2)], [(0, 2), (1, 2)]),
            ("u", [(2, 1), (2, 2)], [(1, 1), (1, 2)]),
        ],
    }
    for name in ORDER:
        if name[0] == "P":
            put(name, *kernels[name])
            continue
        m, kind, sign, q = name[0], name[1], name[2], name[3:]
        on_x = (m == "g") == (kind in "st")
        step = 1 if sign == "+" else 3
        if kind == "s":
            small[m][str(step)] = move(small[m]["0"], on_x, sign)
        elif kind == "t":
            part = small[m][q][:CUT] if sign == "+" else small[m][q][CUT:]
            small[m]["2a" if sign == "+" else "2b"] = move(part, on_x, sign)
        elif kind == "b":
            large[m][(step, q)] = move(small[m][q], on_x, sign)
        elif q == "1a":
            large[m][(2, q)] = move(large[m][(step, "1")][:CUT], on_x, sign)
        elif q == "1b":
            large[m][(2, q)] = move(large[m][(step, "1")][CUT:], on_x, sign)
        else:
            large[m][(2, q)] = move(large[m][(step, q)], on_x, sign)
    return out["g"], out["u"]


def body(train_gate, drift_gate, spread_gate, train_up, drift_up, spread_up, norm_gain):
    hold_gate = hold_rate * drift_gate + spread_gate
    whole_gate = train_gate - learn_rate * hold_gate
    hold_up = hold_rate * drift_up + spread_up
    whole_up = train_up - learn_rate * hold_up
    gained_gate = whole_gate * norm_gain[:, None]
    gained_up = whole_up * norm_gain[:, None]
    tops = jnp.stack([jnp.max(jnp.abs(gained_gate), axis=0), jnp.max(jnp.abs(gained_up), axis=0)])
    tops = lax.all_to_all(jnp.broadcast_to(tops, (SIDE * SIDE, 2, COLS)), "zero", 0, 0, tiled=True)
    gate = packed(gained_gate, tops, 0)
    up = packed(gained_up, tops, 1)
    factor_gate, factor_up = tops[:, 0].max(axis=0), tops[:, 1].max(axis=0)
    serving_gate, serving_up = spread(gate, up)
    return serving_gate.T, serving_up.T, factor_gate.reshape(COLS), factor_up.reshape(COLS)


def solution(mesh):
    return jax.shard_map(
        body,
        mesh=mesh,
        in_specs=(P("zero", "width"),) * 6 + (P("zero"),),
        out_specs=(P(None, "width"), P(None, "width"), P("width"), P("width")),
        check_vma=False,
    )
```

```python
import functools

import jax
import jax.numpy as jnp
from jax import lax
from jax.experimental import pallas as pl
from jax.experimental.pallas import tpu as pltpu
from jax.sharding import PartitionSpec as P


learn_rate = 0.3
hold_rate = 0.9


ROWS = 320
COLS = 864
FULL = 256
HALF = 64
QUART = COLS // 4
PIECE = COLS + QUART
LAST = 624
CUT = 624
SIDE = 4


def pack_kernel(m, w_ref, tops_ref, o_ref):
    odd = lax.axis_index("zero") % 2
    full_at = pl.multiple_of(odd * HALF, 8)
    half_at = pl.multiple_of((1 - odd) * FULL, 8)
    factor = jnp.max(tops_ref[:, m, :], axis=0, keepdims=True)
    for at in range(0, COLS, 128):
        n = min(128, COLS - at)
        w = w_ref[pl.ds(full_at, FULL), at : at + n] / factor[:, at : at + n]
        o_ref[QUART + at : QUART + at + n, :] = w.T.astype(jnp.bfloat16)
    h = w_ref[pl.ds(half_at, HALF), :] / factor
    t = jnp.concatenate([h, h], axis=0).T
    low = lax.broadcasted_iota(jnp.int32, (2 * QUART, 128), 1) < HALF
    keep = jnp.logical_xor(low, odd == 1)
    p = jnp.where(keep, t[: 2 * QUART], t[2 * QUART :]).astype(jnp.bfloat16)
    o_ref[:QUART, :128] = p[:QUART]
    o_ref[:QUART, 128:] = p[QUART:]


def packed(w, tops, m):
    return pl.pallas_call(
        functools.partial(pack_kernel, m),
        out_shape=jax.ShapeDtypeStruct((PIECE, 256), jnp.bfloat16),
        in_specs=[pl.BlockSpec(memory_space=pltpu.VMEM)] * 2,
        out_specs=pl.BlockSpec(memory_space=pltpu.VMEM),
        compiler_params=pltpu.CompilerParams(vmem_limit_bytes=8 << 20),
        cost_estimate=pl.CostEstimate(flops=4_000_000, bytes_accessed=1_600_000, transcendentals=0),
    )(w, tops)


def tile_of(kx, ky):
    i = lax.axis_index("zero")
    x, y = i % SIDE, i // SIDE
    j = ((y + SIDE - ky) % SIDE) * SIDE + (x + SIDE - kx) % SIDE
    return pl.multiple_of((5 * j + j % 2) // 2 * 128, 128)


def pair_tile(kx, ky):
    i = lax.axis_index("zero")
    x, y = i % SIDE, i // SIDE
    j = ((y + SIDE - ky) % SIDE) * SIDE + (x + SIDE - kx) % SIDE
    return pl.multiple_of((5 * (j // 2) + 2) * 128, 128)


def place_kernel(plan, n_in, first, *refs):
    ins, outs = refs[:n_in], refs[n_in + len(plan) * (not first) :][: len(plan)]
    tiles, sem_full, sem_tile = refs[-3:]
    odd = lax.axis_index("zero") % 2
    done = []
    for (layout, fulls, _), out in zip(plan, outs):
        for key, part in fulls:
            at = tile_of(*key)
            for r, a, b in [layout[key, q] for q in part]:
                lo = max(a, QUART)
                if b > lo:
                    c = pltpu.make_async_copy(
                        ins[r].at[pl.ds(lo - a, b - lo), :],
                        out.at[pl.ds(lo - QUART, b - lo), pl.ds(at, FULL)],
                        sem_full.at[len(done)],
                    )
                    c.start()
                    done.append(c)

    keep = jnp.logical_xor(lax.broadcasted_iota(jnp.int32, (QUART, 128), 1) < HALF, odd == 1)
    n_tiles = 0
    for (layout, _, pairs), out in zip(plan, outs):

        def half(key, lanes):
            return ins[layout[key, 0][0]][:QUART, lanes].astype(jnp.float32)

        for p, ky in pairs:
            tile = tiles.at[n_tiles]

            def join(kx):
                for b in range(2):
                    lanes = slice(128 * b, 128 * b + 128)
                    one, two = half((2 * p, ky), lanes), half((kx, ky), lanes)
                    top = jnp.where(keep, one, two)
                    low = pltpu.roll(jnp.where(keep, two, one), HALF, 1)
                    tile[QUART * b : QUART * b + QUART, :] = top.astype(jnp.bfloat16)
                    tile[QUART * b + 2 * QUART : QUART * b + 3 * QUART, :] = low.astype(jnp.bfloat16)

            pl.when(odd == 0)(lambda: join(3 - 2 * p))
            pl.when(odd == 1)(lambda: join(1 + 2 * p))
            c = pltpu.make_async_copy(tile, out.at[:, pl.ds(pair_tile(2 * p, ky), 128)], sem_tile.at[n_tiles])
            c.start()
            done.append(c)
            n_tiles += 1
    for c in done:
        c.wait()


def place(jobs):
    refs, plan = [], []
    for _, got, fulls, pairs in jobs:
        layout = {}
        need = [(key, q) for key, part in fulls for q in part]
        need += [((k, ky), 0) for p, ky in pairs for k in (2 * p, 1, 3)]
        for key, q in need:
            parts = got[key]
            one = parts[q]
            if not any(one is r for r in refs):
                refs.append(one)
            r = [one is x for x in refs].index(True)
            at = sum(x.shape[0] for x in parts[: q % len(parts)])
            layout[key, q] = (r, at, at + one.shape[0])
        plan.append((layout, tuple(fulls), tuple(pairs)))
    first = jobs[0][0] is None
    olds = [] if first else [j[0] for j in jobs]
    n_tiles = max(1, sum(len(j[3]) for j in jobs))
    n_full = max(1, sum(len(part) for _, fulls, _ in plan for _, part in fulls))
    shape = jax.ShapeDtypeStruct((COLS, ROWS * SIDE * SIDE), jnp.bfloat16)
    return pl.pallas_call(
        functools.partial(place_kernel, plan, len(refs), first),
        out_shape=[shape] * len(jobs),
        in_specs=[pl.BlockSpec(memory_space=pltpu.VMEM)] * len(refs) + [pl.BlockSpec(memory_space=pl.ANY)] * len(olds),
        out_specs=[pl.BlockSpec(memory_space=pl.ANY)] * len(jobs),
        scratch_shapes=[
            pltpu.VMEM((n_tiles, COLS, 128), jnp.bfloat16),
            pltpu.SemaphoreType.DMA((n_full,)),
            pltpu.SemaphoreType.DMA((n_tiles,)),
        ],
        input_output_aliases={len(refs) + i: i for i in range(len(olds))},
        compiler_params=pltpu.CompilerParams(vmem_limit_bytes=6 << 20),
        cost_estimate=pl.CostEstimate(flops=1_000_000, bytes_accessed=4_000_000, transcendentals=0),
    )(*refs, *olds)


def shift(a, dx, dy):
    pairs = [
        (SIDE * y + x, SIDE * ((y + dy) % SIDE) + (x + dx) % SIDE) for y in range(SIDE) for x in range(SIDE)
    ]
    return lax.ppermute(a, "zero", pairs)


ORDER = [
    *"gs+0 us+0 gs-0 us-0".split(),
    *"ub+0 gb+0 ub-0 gb-0".split(),
    *"gt+1 ut+1 gt-3 ut-3".split(),
    *"ub+1 gb+1 ub-3 gb-3".split(),
    *"ub+3 gb+3".split(),
    *"ub-2a gb-2a ub-2b gb-2b".split(),
    *"ub+2a gb+2a ub+2b gb+2b".split(),
    *"ub-1 gb-1".split(),
    *"Pg0 Pu0".split(),
    *"uf+0 gf+0 uf-3 gf-3".split(),
    *"uf+1a gf+1a uf-2a gf-2a".split(),
    *"uf+1b gf+1b uf-2b gf-2b".split(),
    *"Pg1 Pu1 Pg3 Pu3".split(),
    *"Pg2 Pu2".split(),
    *"Pmid Pend".split(),
]


def spread(gate, up):
    small = {"g": {"0": gate}, "u": {"0": up}}
    large = {"g": {}, "u": {}}
    out = {"g": None, "u": None}

    def move(a, on_x, sign):
        d = 1 if sign == "+" else -1
        return shift(a, d, 0) if on_x else shift(a, 0, d)

    def pieces(m):
        got = {}
        for step in range(SIDE):
            have = small[m] if step == 0 else {q: v for (s, q), v in large[m].items() if s == step}
            for k in range(SIDE):
                names = [str(k)] if str(k) in have else [f"{k}a", f"{k}b"]
                got[(k, step) if m == "g" else (step, k)] = [have.get(q) for q in names]
        return got

    def whole(m, keys):
        return [(key, tuple(range(len(pieces(m)[key])) if (pieces(m)[key][0] is not None) else ())) for key in keys]

    def put(name, *jobs):
        split = {"Pmid": (0,), "Pend": (1,)}
        res = place(
            [
                (out[m], pieces(m), [(k, split[name]) if name in split else w for k, w in zip(keys, whole(m, keys))], pairs)
                for m, keys, pairs in jobs
            ],
        )
        for (m, _, _), r in zip(jobs, res):
            out[m] = r

    every = range(SIDE)
    kernels = {
        "Pg0": [("g", [(k, 0) for k in every], [(0, 0), (1, 0)])],
        "Pg1": [("g", [(k, 1) for k in every], [(0, 1), (1, 1)])],
        "Pg3": [("g", [(k, 3) for k in every], [(0, 3), (1, 3)])],
        "Pg2": [("g", [(0, 2), (3, 2)], [])],
        "Pu0": [("u", [(0, k) for k in every], [])],
        "Pu1": [("u", [(1, k) for k in every], [])],
        "Pu3": [("u", [(3, k) for k in every], [(0, k) for k in every])],
        "Pu2": [("u", [(2, 0), (2, 3)], [(1, 0), (1, 3)])],
        "Pmid": [
            ("g", [(1, 2), (2, 2)], [(0, 2), (1, 2)]),
            ("u", [(2, 1), (2, 2)], [(1, 1), (1, 2)]),
        ],
        "Pend": [("g", [(1, 2), (2, 2)], []), ("u", [(2, 1), (2, 2)], [])],
    }
    for name in ORDER:
        if name[0] == "P":
            put(name, *kernels[name])
            continue
        m, kind, sign, q = name[0], name[1], name[2], name[3:]
        on_x = (m == "g") == (kind in "st")
        step = 1 if sign == "+" else 3
        if kind == "s":
            small[m][str(step)] = move(small[m]["0"], on_x, sign)
        elif kind == "t":
            part = small[m][q][:CUT] if sign == "+" else small[m][q][CUT:]
            small[m]["2a" if sign == "+" else "2b"] = move(part, on_x, sign)
        elif kind == "b":
            large[m][(step, q)] = move(small[m][q], on_x, sign)
        elif q == "1a":
            large[m][(2, q)] = move(large[m][(step, "1")][:LAST], on_x, sign)
        elif q == "1b":
            large[m][(2, q)] = move(large[m][(step, "1")][LAST:], on_x, sign)
        else:
            large[m][(2, q)] = move(large[m][(step, q)], on_x, sign)
    return out["g"], out["u"]


def body(train_gate, drift_gate, spread_gate, train_up, drift_up, spread_up, norm_gain):
    hold_gate = hold_rate * drift_gate + spread_gate
    whole_gate = train_gate - learn_rate * hold_gate
    hold_up = hold_rate * drift_up + spread_up
    whole_up = train_up - learn_rate * hold_up
    gained_gate = whole_gate * norm_gain[:, None]
    gained_up = whole_up * norm_gain[:, None]
    tops = jnp.stack([jnp.max(jnp.abs(gained_gate), axis=0), jnp.max(jnp.abs(gained_up), axis=0)])
    tops = lax.all_to_all(jnp.broadcast_to(tops, (SIDE * SIDE, 2, COLS)), "zero", 0, 0, tiled=True)
    gate = packed(gained_gate, tops, 0)
    up = packed(gained_up, tops, 1)
    factor_gate, factor_up = tops[:, 0].max(axis=0), tops[:, 1].max(axis=0)
    serving_gate, serving_up = spread(gate, up)
    return serving_gate.T, serving_up.T, factor_gate.reshape(COLS), factor_up.reshape(COLS)


def solution(mesh):
    return jax.shard_map(
        body,
        mesh=mesh,
        in_specs=(P("zero", "width"),) * 6 + (P("zero"),),
        out_specs=(P(None, "width"), P(None, "width"), P("width"), P("width")),
        check_vma=False,
    )
```
